8 devices in a mesh: data: 2 (over z, y), dap: 4 (over x, core).
Axes of the slice: x: 2, y: 2, z: 1, core: 2. Of those that a mesh axis runs over, the one named last changes fastest.
Arguments:
- pair_act: float32 [512, 256, 128], P(('data', 'dap')), parts along dimension 0
- pair_mask: int32 [512, 256], P(('data', 'dap')), parts along dimension 0
- grad_out: float32 [512, 256, 128], P(('data', 'dap')), parts along dimension 0
- ln_pair: bfloat16 [2, 2, 128], replicated
- w_in: bfloat16 [2, 128, 640], replicated
- ln_tri: bfloat16 [2, 2, 128], replicated
- w_out: bfloat16 [2, 128, 128], replicated
Outputs:
- output 1: float32 [512, 256, 128], P(('data', 'dap')), parts along dimension 0
- output 2: float32 [4, 2, 128], P('data'), parts along dimension 0
- output 3: float32 [4, 128, 640], P('data'), parts along dimension 0
- output 4: float32 [4, 2, 128], P('data'), parts along dimension 0
- output 5: float32 [4, 128, 128], P('data'), parts along dimension 0
There are 2 independent parts. The reference program is written for one: setup_inputs(seed, part) draws one part's arguments, and reference() takes and returns one part's arrays. A program takes and returns all parts, laid end to end along the dimension named above; an argument that names none is the same for every part.
All inputs are finite; a program needn't handle non-finite values.
Results may differ from the reference program's by a relative error of at most 0.014421.
Values are sent between devices in bfloat16 or wider.
A program may use at most 1 GiB of HBM per device.

```python
import jax
import jax.numpy as jnp
from jax import lax

PAIR_DIM = 128
HIDDEN = 128
ROWS_DEV = 64
GROUP_SIZE = 4
SEQ_LEN = ROWS_DEV * GROUP_SIZE
LN_EPS = 1e-5
OUT_FORM = 'ikc,jkc->ijc'
IN_FORM = 'kic,kjc->ijc'


def setup_inputs(seed: int = 0, part: int = 0) -> dict:
    part_keys = jax.random.split(jax.random.fold_in(jax.random.key(seed), part), 3)
    shared_keys = jax.random.split(jax.random.key(seed + 1), 6)
    width_in = 4 * HIDDEN + PAIR_DIM
    pair_act = jax.random.normal(part_keys[0], (SEQ_LEN, SEQ_LEN, PAIR_DIM), jnp.float32)
    tail_len = jax.random.randint(part_keys[1], (), SEQ_LEN // 16 + 1, SEQ_LEN // 8 + 2)
    seq_mask = (jnp.arange(SEQ_LEN) < SEQ_LEN - tail_len).astype(jnp.int32)
    pair_mask = seq_mask[:, None] * seq_mask[None, :]
    grad_out = jax.random.normal(part_keys[2], (SEQ_LEN, SEQ_LEN, PAIR_DIM), jnp.float32)
    gain_pair = 1.0 + 0.3 * jax.random.normal(shared_keys[0], (2, 1, PAIR_DIM), jnp.float32)
    bias_pair = 0.3 * jax.random.normal(shared_keys[1], (2, 1, PAIR_DIM), jnp.float32)
    w_in = jax.random.normal(shared_keys[2], (2, PAIR_DIM, width_in), jnp.float32) * PAIR_DIM ** -0.5
    gain_tri = 1.0 + 0.3 * jax.random.normal(shared_keys[3], (2, 1, HIDDEN), jnp.float32)
    bias_tri = 0.3 * jax.random.normal(shared_keys[4], (2, 1, HIDDEN), jnp.float32)
    w_out = jax.random.normal(shared_keys[5], (2, HIDDEN, PAIR_DIM), jnp.float32) * HIDDEN ** -0.5
    return {
        'pair_act': pair_act,
        'pair_mask': pair_mask,
        'grad_out': grad_out,
        'ln_pair': jnp.concatenate([gain_pair, bias_pair], axis=1).astype(jnp.bfloat16),
        'w_in': w_in.astype(jnp.bfloat16),
        'ln_tri': jnp.concatenate([gain_tri, bias_tri], axis=1).astype(jnp.bfloat16),
        'w_out': w_out.astype(jnp.bfloat16),
    }


def layer_norm(values, gain_vec, bias_vec):
    mean_val = jnp.mean(values, axis=-1, keepdims=True)
    centred = values - mean_val
    variance = jnp.mean(centred * centred, axis=-1, keepdims=True)
    return centred * lax.rsqrt(variance + LN_EPS) * gain_vec + bias_vec


def project_rows(row_vals, mask_rows, ln_pair, w_in):
    normed = layer_norm(row_vals, ln_pair[0], ln_pair[1]).astype(jnp.bfloat16)
    proj_all = jnp.einsum('ijc,cd->ijd', normed.astype(jnp.float32), w_in)
    mask_f = mask_rows.astype(jnp.float32)[:, :, None]
    left_act = (mask_f * jax.nn.sigmoid(proj_all[:, :, HIDDEN:2 * HIDDEN]) * proj_all[:, :, :HIDDEN]).astype(jnp.bfloat16)
    right_act = (mask_f * jax.nn.sigmoid(proj_all[:, :, 3 * HIDDEN:4 * HIDDEN]) * proj_all[:, :, 2 * HIDDEN:3 * HIDDEN]).astype(jnp.bfloat16)
    gate_act = jax.nn.sigmoid(proj_all[:, :, 4 * HIDDEN:])
    return left_act, right_act, gate_act


def finish_rows(row_vals, tri_sum, gate_act, ln_tri, w_out):
    tri_norm = layer_norm(tri_sum, ln_tri[0], ln_tri[1]).astype(jnp.bfloat16)
    return row_vals + gate_act * jnp.einsum('ijc,cd->ijd', tri_norm.astype(jnp.float32), w_out)


def tri_update(pair_act, pair_mask, ln_pair, w_in, ln_tri, w_out, ein_form):
    block_shape = (GROUP_SIZE, ROWS_DEV, SEQ_LEN)
    pair_blocks = pair_act.reshape(block_shape + (PAIR_DIM,))
    left_act, right_act, gate_act = lax.map(
        jax.checkpoint(lambda row_block: project_rows(row_block[0], row_block[1], ln_pair, w_in)),
        (pair_blocks, pair_mask.reshape(block_shape)))
    tri_sum = jnp.einsum(ein_form,
                         left_act.reshape(SEQ_LEN, SEQ_LEN, HIDDEN).astype(jnp.float32),
                         right_act.reshape(SEQ_LEN, SEQ_LEN, HIDDEN).astype(jnp.float32))
    new_blocks = lax.map(
        jax.checkpoint(lambda row_block: finish_rows(row_block[0], row_block[1], row_block[2], ln_tri, w_out)),
        (pair_blocks, tri_sum.reshape(block_shape + (HIDDEN,)), gate_act))
    return new_blocks.reshape(SEQ_LEN, SEQ_LEN, PAIR_DIM)


def block_forward(pair_act, pair_mask, ln_pair, w_in, ln_tri, w_out):
    mid_act = tri_update(pair_act, pair_mask, ln_pair[0], w_in[0], ln_tri[0], w_out[0], OUT_FORM)
    return tri_update(mid_act, pair_mask, ln_pair[1], w_in[1], ln_tri[1], w_out[1], IN_FORM)


def reference(pair_act, pair_mask, grad_out, ln_pair, w_in, ln_tri, w_out):
    def forward(pair_in, ln_pair_v, w_in_v, ln_tri_v, w_out_v):
        return block_forward(pair_in, pair_mask, ln_pair_v, w_in_v, ln_tri_v, w_out_v)
    pull_back = jax.vjp(forward, pair_act, ln_pair.astype(jnp.float32), w_in.astype(jnp.float32),
                        ln_tri.astype(jnp.float32), w_out.astype(jnp.float32))[1]
    grad_all = pull_back(grad_out)
    return (grad_all[0], grad_all[1], grad_all[2], grad_all[3], grad_all[4])
```

```python
import jax
import jax.numpy as jnp
from jax import lax
from jax.experimental import pallas as pl
from jax.experimental.pallas import tpu as pltpu
from jax.sharding import PartitionSpec as P


LN_EPS = 1e-5
C = 128
HALF = 128
ROWS = 64
RB = 16
CB = 16
F32 = jnp.float32
BF16 = jnp.bfloat16


def mm(a, b):
    return lax.dot_general(a, b, (((1,), (0,)), ((), ())), preferred_element_type=F32)


def mm_nt(a, b):
    return lax.dot_general(a, b, (((1,), (1,)), ((), ())), preferred_element_type=F32)


def mm_tn(a, b):
    return lax.dot_general(a, b, (((0,), (0,)), ((), ())), preferred_element_type=F32)


def sigmoid(x):
    return 0.5 * jnp.tanh(0.5 * x) + 0.5


def mean0(x):
    return jnp.sum(x, axis=0, keepdims=True) * (1.0 / C)


def normalise(x):
    cen = x - mean0(x)
    rstd = lax.rsqrt(mean0(cen * cen) + LN_EPS)
    return cen * rstd, rstd


def norm_back(d_f, gain, hat, rstd):
    dg = d_f * gain
    return rstd * (dg - mean0(dg) - hat * mean0(dg * hat))


def pair(ref, r):
    return jnp.concatenate([ref[r], ref[r + 1]], axis=1)


def pair_t(ref, r):
    return jnp.concatenate([ref[r].T, ref[r + 1].T], axis=1)


def pair_cm(flat, r):
    return jnp.concatenate([flat[pl.ds(r, C, stride=RB), :],
                            flat[pl.ds(r + 1, C, stride=RB), :]], axis=1)


def put_pair(ref, r, val):
    ref[r] = val[:, :HALF]
    ref[r + 1] = val[:, HALF:]


def put_pair_cm(flat, r, val):
    flat[pl.ds(r, C, stride=RB), :] = val[:, :HALF]
    flat[pl.ds(r + 1, C, stride=RB), :] = val[:, HALF:]


def pair_mask(ref, r):
    return jnp.concatenate([ref[pl.ds(r, 1), :], ref[pl.ds(r + 1, 1), :]], axis=1)


def twice(v):
    return jnp.concatenate([v, v], axis=1)


def loop_units(body):
    def step(u, _):
        body(u * 2)
        return 0

    lax.fori_loop(0, RB // 2, step, 0, unroll=2)


def zero_at_start(refs):
    @pl.when(pl.program_id(0) == 0)
    def _():
        for ref in refs:
            ref[...] = jnp.zeros_like(ref)


def norm_kernel(info, z, mask, lnb, zn, znm):
    def unit(r):
        zt = pair_t(z, r)
        hat, _ = normalise(zt)
        val = hat * twice(lnb[0]) + twice(lnb[1])
        put_pair(zn, r, val.astype(BF16))
        put_pair(znm, r, (val * pair_mask(mask, r)).astype(BF16))

    loop_units(unit)


def proj_kernel(znm, w_t, a_out, b_out, a_s, b_s):
    def unit(r):
        zv = pair(znm, r)
        p = mm(w_t[...], zv)
        put_pair_cm(a_s, r, p[0:C] * sigmoid(p[C:2 * C]))
        put_pair_cm(b_s, r, p[2 * C:3 * C] * sigmoid(p[3 * C:4 * C]))

    loop_units(unit)
    a_out[...] = a_s[...].reshape(C, RB, HALF).astype(BF16)
    b_out[...] = b_s[...].reshape(C, RB, HALF).astype(BF16)


def tri_out_kernel(info, a, b, x):
    def body(c, _):
        x[c] = mm_nt(a[c], b[c])
        return 0

    lax.fori_loop(0, CB, body, 0, unroll=4)


def finish_mid_kernel(info, x, zn, z, mask, lnb, wo_t, wg_t, z1, zn1, zn1m, xf):
    xf[...] = x[...].reshape(C * RB, HALF)

    def unit(r):
        hat, _ = normalise(pair_cm(xf, r))
        xn = (hat * twice(lnb[0]) + twice(lnb[1])).astype(BF16)
        out = mm(wo_t[...], xn)
        gate = sigmoid(mm(wg_t[...], pair(zn, r)))
        new = pair_t(z, r) + gate * out
        put_pair(z1, r, new)
        hat1, _ = normalise(new)
        val = hat1 * twice(lnb[2]) + twice(lnb[3])
        put_pair(zn1, r, val.astype(BF16))
        put_pair(zn1m, r, (val * pair_mask(mask, r)).astype(BF16))

    loop_units(unit)


def tri_in_kernel(info, a_s, a_r, bs0, bs1, br0, br1, x0, x1, tmp):
    off = pl.multiple_of(info[1] * ROWS, ROWS)

    def body(c, _):
        lhs = jnp.concatenate([a_s[c], a_r[c]], axis=0)
        rhs = jnp.concatenate([jnp.concatenate([bs0[c], bs1[c]], axis=1),
                               jnp.concatenate([br0[c], br1[c]], axis=1)], axis=0)
        tmp[c] = mm_tn(lhs, rhs)
        x0[c] = tmp[c, pl.ds(off, ROWS), :HALF]
        x1[c] = tmp[c, pl.ds(off, ROWS), HALF:]
        return 0

    lax.fori_loop(0, CB, body, 0, unroll=4)


def finish_back_unit(d_new, x_val, zn_val, gain, bias, wo_t, wo, wg_t, gw, gg, gb):
    hat, rstd = normalise(x_val)
    xn = (hat * gain + bias).astype(BF16)
    out = mm(wo_t[...], xn)
    gate = sigmoid(mm(wg_t[...], zn_val))
    d_proj_f = d_new * gate
    d_gate = (d_proj_f * out * (1.0 - gate)).astype(BF16)
    d_proj = d_proj_f.astype(BF16)
    gw[...] += mm_nt(xn, d_proj)
    d_norm = mm(wo[...], d_proj).astype(BF16).astype(F32)
    gg[...] += d_norm * hat
    gb[...] += d_norm
    return norm_back(d_norm, gain, hat, rstd), d_gate


def finish_back_kernel(info, x, zn, g, lnb, wo_t, wo, wg_t, dx, dqg, gw, gg, gb, dx_s, xf):
    zero_at_start((gw, gg, gb))
    xf[...] = x[...].reshape(C * RB, HALF)

    def unit(r):
        d_x, d_gate = finish_back_unit(pair_t(g, r), pair_cm(xf, r), pair(zn, r), twice(lnb[0]),
                                       twice(lnb[1]), wo_t, wo, wg_t, gw, gg, gb)
        put_pair(dqg, r, d_gate)
        put_pair_cm(dx_s, r, d_x)

    loop_units(unit)
    dx[...] = dx_s[...].reshape(C, RB, HALF).astype(BF16)


def tri_in_back_kernel(info, a0, a1, b0, b1, s0, s1, r0, r1, da0, da1, db0, db1):
    def body(c, _):
        cols0 = jnp.concatenate([s0[0, c], s0[1, c], r0[0, c], r0[1, c]], axis=0)
        cols1 = jnp.concatenate([s1[0, c], s1[1, c], r1[0, c], r1[1, c]], axis=0)
        d_all = jnp.concatenate([cols0, cols1], axis=1)
        d_a = mm_nt(jnp.concatenate([b0[c], b1[c]], axis=1), d_all).astype(BF16)
        d_b = mm(jnp.concatenate([a0[c], a1[c]], axis=1), d_all).astype(BF16)
        da0[c] = d_a[:, :HALF]
        da1[c] = d_a[:, HALF:]
        db0[c] = d_b[:, :HALF]
        db1[c] = d_b[:, HALF:]
        return 0

    lax.fori_loop(0, CB, body, 0, unroll=2)


def project_back_unit(d_a, d_b, d_gate, zn_val, m, w_t, w, gain, hat, rstd, gw, gg, gb):
    p = mm(w_t[...], zn_val)
    d_a = d_a * m
    d_b = d_b * m
    sig_a = sigmoid(p[C:2 * C])
    sig_b = sigmoid(p[3 * C:4 * C])
    da_sig = d_a * sig_a
    db_sig = d_b * sig_b
    d_cat = jnp.concatenate([
        da_sig.astype(BF16), (da_sig * p[0:C] * (1.0 - sig_a)).astype(BF16),
        db_sig.astype(BF16), (db_sig * p[2 * C:3 * C] * (1.0 - sig_b)).astype(BF16), d_gate], axis=0)
    gw[...] += mm_nt(d_cat, zn_val)
    d_zn = mm(w[...], d_cat).astype(BF16).astype(F32)
    gg[...] += d_zn * hat
    gb[...] += d_zn
    return norm_back(d_zn, gain, hat, rstd)


def back_mid_kernel(info, da, db, dqg, zn1, z1, mask, g, x, zn, lnb, w1_t, w1, wo_t, wo, wg_t,
                    d_mid, dx, dqg0, gw1, gg1, gb1, gwo, ggo, gbo, da_s, db_s, dx_s, xf):
    zero_at_start((gw1, gg1, gb1, gwo, ggo, gbo))
    da_s[...] = da[...].astype(F32).reshape(C * RB, HALF)
    db_s[...] = db[...].astype(F32).reshape(C * RB, HALF)
    xf[...] = x[...].reshape(C * RB, HALF)

    def unit(r):
        hat1, rstd1 = normalise(pair(z1, r))
        d_ln = project_back_unit(pair_cm(da_s, r), pair_cm(db_s, r), pair(dqg, r), pair(zn1, r),
                                 pair_mask(mask, r), w1_t, w1, twice(lnb[2]), hat1, rstd1, gw1, gg1, gb1)
        d_new = pair_t(g, r) + d_ln
        put_pair(d_mid, r, d_new)
        d_x, d_gate = finish_back_unit(d_new, pair_cm(xf, r), pair(zn, r), twice(lnb[0]),
                                       twice(lnb[1]), wo_t, wo, wg_t, gwo, ggo, gbo)
        put_pair(dqg0, r, d_gate)
        put_pair_cm(dx_s, r, d_x)

    loop_units(unit)
    dx[...] = dx_s[...].reshape(C, RB, HALF).astype(BF16)


def tri_out_back_kernel(info, d0, d1, b_s, b_r, s, r, a_s, a_r, da, db, tmp):
    off = pl.multiple_of(info[1] * ROWS, ROWS)

    def body(c, _):
        d_own = jnp.concatenate([d0[c], d1[c]], axis=1)
        b_all = jnp.concatenate([b_s[c], b_r[c]], axis=0)
        a_all = jnp.concatenate([a_s[c], a_r[c]], axis=0)
        d_col = jnp.concatenate([s[0, c], s[1, c], r[0, c], r[1, c]], axis=0)
        da[c] = mm(d_own, b_all).astype(BF16)
        tmp[c] = mm_tn(d_col, a_all)
        db[c] = tmp[c, pl.ds(off, ROWS), :].astype(BF16)
        return 0

    lax.fori_loop(0, CB, body, 0, unroll=2)


def back_out_body(da, db, dqg, zn, z, mask, d_mid, lnb, w_t, w, out, gw, gg, gb, da_s, db_s):
    zero_at_start((gw, gg, gb))
    da_s[...] = da[...].astype(F32).reshape(C * RB, HALF)
    db_s[...] = db[...].astype(F32).reshape(C * RB, HALF)

    def unit(r):
        hat, rstd = normalise(pair_t(z, r))
        d_ln = project_back_unit(pair_cm(da_s, r), pair_cm(db_s, r), pair(dqg, r), pair(zn, r),
                                 pair_mask(mask, r), w_t, w, twice(lnb[0]), hat, rstd, gw, gg, gb)
        res = pair(d_mid, r) + d_ln
        out[r] = res[:, :HALF].T
        out[r + 1] = res[:, HALF:].T

    loop_units(unit)


def back_out_kernel(info, *refs):
    back_out_body(*refs)


def back_out_second_kernel(info, prev, *refs):
    back_out_body(*refs)


def sds(shape, dtype):
    return jax.ShapeDtypeStruct(shape, dtype)


def call(body, info, args, grid, in_specs, outs, out_specs, scratch=(), flops=0, nbytes=0, aliases={}):
    spec = pltpu.PrefetchScalarGridSpec(num_scalar_prefetch=1, grid=grid, in_specs=in_specs,
                                        out_specs=out_specs, scratch_shapes=list(scratch))
    return pl.pallas_call(
        body, out_shape=outs, grid_spec=spec, input_output_aliases=aliases,
        compiler_params=pltpu.CompilerParams(dimension_semantics=('arbitrary',) * len(grid)),
        cost_estimate=pl.CostEstimate(flops=flops, bytes_accessed=nbytes, transcendentals=0))(info, *args)


def whole(arr):
    nd = arr.ndim
    return pl.BlockSpec(arr.shape, lambda *_: (0,) * nd)


ROWS_T = pl.BlockSpec((RB, C, HALF), lambda i, s: (i, 0, 0))
CM = pl.BlockSpec((C, RB, HALF), lambda i, s: (0, i, 0))
CM_OUT = sds((C, ROWS, HALF), BF16)
ROW_OUT = sds((ROWS, C, HALF), BF16)
SCR = pltpu.VMEM((C * RB, HALF), F32)
US = 4_000_000


def tok_spec(h):
    return pl.BlockSpec((RB, HALF, C), lambda i, s: (i, s[0] ^ h, 0))


def rowcol_spec(h):
    return pl.BlockSpec((RB, C, HALF), lambda i, s: (i, 0, s[0] ^ h))


def mask_spec(h):
    return pl.BlockSpec((RB, HALF), lambda i, s: (i, s[0] ^ h))


def cm_abs_spec(h):
    return pl.BlockSpec((C, RB, HALF), lambda i, s: (0, i, s[0] ^ h))


def acc(rows, cols):
    return sds((rows, cols), F32), pl.BlockSpec((rows, cols), lambda *_: (0, 0))


def run_norm(info, z, mask, lnb):
    row2 = pl.BlockSpec((RB, C, HALF), lambda i, j, s: (i, 0, j))
    return call(norm_kernel, info, (z, mask, lnb), (ROWS // RB, 2),
                [pl.BlockSpec((RB, HALF, C), lambda i, j, s: (i, j, 0)),
                 pl.BlockSpec((RB, HALF), lambda i, j, s: (i, j)), whole(lnb)],
                [sds((ROWS, C, 2 * HALF), BF16)] * 2, [row2] * 2, flops=15 * US, nbytes=16 << 20)


def run_proj(info, znm, w_t):
    rows, _, cols = znm.shape
    cm2 = pl.BlockSpec((C, RB, HALF), lambda i, j, s: (0, i, j))
    return call(lambda info, *refs: proj_kernel(*refs), info, (znm, w_t), (rows // RB, cols // HALF),
                [pl.BlockSpec((RB, C, HALF), lambda i, j, s: (i, 0, j)), whole(w_t)],
                [sds((C, rows, cols), BF16)] * 2, [cm2] * 2, scratch=[SCR, SCR],
                flops=(rows * cols // 2048) * US, nbytes=rows * cols * C * 6)


def run_tri_out(info, a, b):
    return call(tri_out_kernel, info, (a, b), (C // CB,),
                [pl.BlockSpec((CB, ROWS, 2 * HALF), lambda i, s: (i, s[1], 0)),
                 pl.BlockSpec((CB, HALF, 2 * HALF), lambda i, s: (i, 0, 0))],
                sds((C, ROWS, HALF), F32), pl.BlockSpec((CB, ROWS, HALF), lambda i, s: (i, 0, 0)),
                flops=6 * US, nbytes=16 << 20)


def run_finish_mid(info, h, x, zn, z, mask, lnb, wo_t, wg_t):
    return call(finish_mid_kernel, info, (x, zn, z, mask, lnb, wo_t, wg_t), (ROWS // RB,),
                [CM, rowcol_spec(h), tok_spec(h), mask_spec(h), whole(lnb), whole(wo_t), whole(wg_t)],
                [sds((ROWS, C, HALF), F32), ROW_OUT, ROW_OUT], [ROWS_T] * 3, scratch=[SCR], flops=14 * US, nbytes=18 << 20)


def run_tri_in(info, a_s, a_r, bs0, bs1, br0, br1):
    full = pl.BlockSpec((CB, HALF, HALF), lambda i, s: (i, 0, 0))
    part = pl.BlockSpec((CB, ROWS, HALF), lambda i, s: (i, 0, 0))
    return call(tri_in_kernel, info, (a_s, a_r, bs0, bs1, br0, br1), (C // CB,), [full] * 6,
                [sds((C, ROWS, HALF), F32)] * 2, [part] * 2,
                scratch=[pltpu.VMEM((CB, HALF, 2 * HALF), F32)], flops=15 * US, nbytes=32 << 20)


def run_finish_back(info, h, x, zn, g, lnb, wo_t, wo, wg_t):
    a1, a2 = acc(C, C), acc(C, 2 * HALF)
    return call(finish_back_kernel, info, (x, zn, g, lnb, wo_t, wo, wg_t), (ROWS // RB,),
                [CM, ROWS_T, tok_spec(h), whole(lnb), whole(wo_t), whole(wo), whole(wg_t)],
                [CM_OUT, ROW_OUT, a1[0], a2[0], a2[0]], [CM, ROWS_T, a1[1], a2[1], a2[1]],
                scratch=[SCR] * 2, flops=16 * US, nbytes=16 << 20)


def run_tri_in_back(info, a0, a1, b0, b1, s0, s1, r0, r1):
    own = pl.BlockSpec((CB, ROWS, HALF), lambda i, s: (i, s[1], 0))
    gat = pl.BlockSpec((2, CB, ROWS, HALF), lambda i, s: (0, i, 0, 0))
    part = pl.BlockSpec((CB, ROWS, HALF), lambda i, s: (i, 0, 0))
    return call(tri_in_back_kernel, info, (a0, a1, b0, b1, s0, s1, r0, r1), (C // CB,),
                [own] * 4 + [gat] * 4, [CM_OUT] * 4, [part] * 4, flops=14 * US, nbytes=32 << 20)


def run_back_mid(info, h, da, db, dqg, zn1, z1, mask, g, x, zn, lnb, w1_t, w1, wo_t, wo, wg_t):
    a1, a2, a3 = acc(5 * C, C), acc(C, 2 * HALF), acc(C, C)
    return call(back_mid_kernel, info, (da, db, dqg, zn1, z1, mask, g, x, zn, lnb, w1_t, w1, wo_t, wo, wg_t),
                (ROWS // RB,),
                [CM, CM, ROWS_T, ROWS_T, ROWS_T, mask_spec(h), tok_spec(h), CM, rowcol_spec(h),
                 whole(lnb), whole(w1_t), whole(w1), whole(wo_t), whole(wo), whole(wg_t)],
                [sds((ROWS, C, HALF), F32), CM_OUT, ROW_OUT, a1[0], a2[0], a2[0], a3[0], a2[0], a2[0]],
                [ROWS_T, CM, ROWS_T, a1[1], a2[1], a2[1], a3[1], a2[1], a2[1]],
                scratch=[SCR] * 4, flops=32 * US, nbytes=32 << 20)


def run_tri_out_back(info, d0, d1, b_s, b_r, s, r, a_s, a_r):
    part = pl.BlockSpec((CB, ROWS, HALF), lambda i, s: (i, 0, 0))
    full = pl.BlockSpec((CB, HALF, 2 * HALF), lambda i, s: (i, 0, 0))
    gat = pl.BlockSpec((2, CB, ROWS, HALF), lambda i, s: (0, i, 0, 0))
    res = pl.BlockSpec((CB, ROWS, 2 * HALF), lambda i, s: (i, 0, 0))
    return call(tri_out_back_kernel, info, (d0, d1, b_s, b_r, s, r, a_s, a_r), (C // CB,),
                [part, part, full, full, gat, gat, full, full],
                [sds((C, ROWS, 2 * HALF), BF16)] * 2, [res] * 2,
                scratch=[pltpu.VMEM((CB, HALF, 2 * HALF), F32)], flops=18 * US, nbytes=48 << 20)


def run_back_out(info, h, prev, da, db, dqg, zn, z, mask, d_mid, lnb, w_t, w):
    a1, a2 = acc(5 * C, C), acc(C, 2 * HALF)
    args = (da, db, dqg, zn, z, mask, d_mid, lnb, w_t, w)
    specs = [cm_abs_spec(h), cm_abs_spec(h), ROWS_T, rowcol_spec(h), tok_spec(h), mask_spec(h), ROWS_T,
             whole(lnb), whole(w_t), whole(w)]
    body, aliases = back_out_kernel, {}
    if prev is not None:
        args, specs = (prev,) + args, [pl.BlockSpec(memory_space=pl.ANY)] + specs
        body, aliases = back_out_second_kernel, {1: 0}
    return call(body, info, args, (ROWS // RB,), specs,
                [sds((ROWS, 2 * HALF, C), F32), a1[0], a2[0], a2[0]],
                [tok_spec(h), a1[1], a2[1], a2[1]], scratch=[SCR] * 2, flops=20 * US, nbytes=24 << 20,
                aliases=aliases)


def lanes(v):
    return jnp.broadcast_to(v.astype(F32)[:, :, None], v.shape + (HALF,))


def solution(mesh):
    row_spec = P(('data', 'dap'))
    grad_spec = P('data')
    cross = [(0, 2), (1, 3), (2, 0), (3, 1)]
    chips = [[0, 1], [2, 3]]

    def swap(v):
        return lax.ppermute(v, 'dap', cross)

    def after(v, *first):
        return lax.optimization_barrier((v,) + first)[0]

    def chip_rows(v):
        return lax.all_gather(v, 'dap', axis=0, tiled=True, axis_index_groups=chips)

    def chip_stack(v):
        return lax.all_gather(v, 'dap', axis=0, tiled=False, axis_index_groups=chips)

    def device_body(z, pair_mask_i, g, ln_pair, w_in, ln_tri, w_out):
        idx = lax.axis_index('dap')
        info = jnp.stack([idx // 2, idx % 2]).astype(jnp.int32)
        mask = pair_mask_i.astype(F32)
        w_t = jnp.swapaxes(w_in, 1, 2)
        wo_t = jnp.swapaxes(w_out, 1, 2)
        wab_t, wabp_t, wg_t = w_t[:, :4 * C], w_t[:, :4 * C], w_t[:, 4 * C:]
        lp0, lp1 = lanes(ln_pair[0]), lanes(ln_pair[1])
        lt0, lt1 = lanes(ln_tri[0]), lanes(ln_tri[1])
        ln_mid = jnp.concatenate([lt0, lp1])

        zn, znm = run_norm(info, z, mask, lp0)
        znm_x = swap(znm)
        a_s, b_s = run_proj(info, chip_rows(znm), wab_t[0])
        x_0 = run_tri_out(info, a_s, b_s)
        z1_0, zn1_0, zn1m_0 = run_finish_mid(info, 0, x_0, zn, z, mask, ln_mid, wo_t[0], wg_t[0])
        n0_x = swap(zn1m_0)
        a_r, b_r = run_proj(info, chip_rows(after(znm_x, zn1m_0)), wab_t[0])
        x_1 = run_tri_out(info, a_s, b_r)
        z1_1, zn1_1, zn1m_1 = run_finish_mid(info, 1, x_1, zn, z, mask, ln_mid, wo_t[0], wg_t[0])
        n1_x = swap(zn1m_1)

        as0, bs0 = run_proj(info, chip_rows(zn1m_0), wab_t[1])
        as1, bs1 = run_proj(info, chip_rows(zn1m_1), wab_t[1])
        _, br1 = run_proj(info, chip_rows(after(n0_x, zn1m_1)), wab_t[1])
        ar0, br0 = run_proj(info, chip_rows(after(n1_x, bs0, bs1, br1)), wab_t[1])
        y_0, y_1 = run_tri_in(info, as0, ar0, bs0, bs1, br0, br1)

        dy_0, dqg1_0, gwo1a, gto1a, bto1a = run_finish_back(info, 0, y_0, zn1_0, g, lt1, wo_t[1], w_out[1], wg_t[1])
        dy0_x = swap(dy_0)
        dy_1, dqg1_1, gwo1b, gto1b, bto1b = run_finish_back(info, 1, y_1, zn1_1, g, lt1, wo_t[1], w_out[1], wg_t[1])
        dy1_x = swap(dy_1)
        da_0, da_1, db_0, db_1 = run_tri_in_back(info, as0, as1, bs0, bs1, chip_stack(dy_0), chip_stack(dy_1),
                                                 chip_stack(dy1_x), chip_stack(after(dy0_x, dy_1)))

        def mid(h, da, db, dqg, zn1, z1, x):
            return run_back_mid(info, h, da, db, dqg, zn1, z1, mask, g, x, zn, ln_mid, wabp_t[1], w_in[1],
                                wo_t[0], w_out[0], wg_t[0])

        dm_1, dx_1, dqg0_1, gwi1b, gpi1b, bpi1b, gwo0b, gto0b, bto0b = mid(1, da_1, db_1, dqg1_1, zn1_1, z1_1, x_1)
        dx1_x = swap(dx_1)
        dm_0, dx_0, dqg0_0, gwi1a, gpi1a, bpi1a, gwo0a, gto0a, bto0a = mid(0, da_0, db_0, dqg1_0, zn1_0, z1_0, x_0)

        da, db = run_tri_out_back(info, dx_0, dx_1, b_s, b_r, chip_stack(dx_0), chip_stack(after(dx1_x, dx_0)), a_s, a_r)
        half, gwi0a, gpi0a, bpi0a = run_back_out(info, 0, None, da, db, dqg0_0, zn, z, mask, dm_0, lp0,
                                                 wabp_t[0], w_in[0])
        res, gwi0b, gpi0b, bpi0b = run_back_out(info, 1, half, da, db, dqg0_1, zn, z, mask, dm_1, lp0,
                                                wabp_t[0], w_in[0])

        def two(ga, gb_, ba, bb):
            return jnp.stack([jnp.sum(ga + gb_, axis=1), jnp.sum(ba + bb, axis=1)])

        first = lax.psum((two(gpi1a, gpi1b, bpi1a, bpi1b), (gwi1a + gwi1b).T,
                          jnp.stack([two(gto0a, gto0b, bto0a, bto0b), two(gto1a, gto1b, bto1a, bto1b)]),
                          jnp.stack([gwo0a + gwo0b, gwo1a + gwo1b])), 'dap')
        last = lax.psum((two(gpi0a, gpi0b, bpi0a, bpi0b), (gwi0a + gwi0b).T), 'dap')
        return (res, jnp.stack([last[0], first[0]]), jnp.stack([last[1], first[1]]), first[2], first[3])

    return jax.shard_map(device_body, mesh=mesh,
                         in_specs=(row_spec, row_spec, row_spec, P(), P(), P(), P()),
                         out_specs=(row_spec, grad_spec, grad_spec, grad_spec, grad_spec),
                         check_vma=False)
```
